16 devices in a mesh: data: 4 (over z, y), seq: 4 (over x, core).
Axes of the slice: x: 2, y: 2, z: 2, core: 2. Of those that a mesh axis runs over, the one named last changes fastest.
Arguments:
- act_in: bfloat16 [256, 1024, 512], P('data', 'seq'), parts along dimension 0
- grad_out: bfloat16 [256, 1024, 512], P('data', 'seq'), parts along dimension 0
- ln1_scale: float32 [512], replicated
- ln1_shift: float32 [512], replicated
- w_tok1: bfloat16 [1024, 256], replicated
- b_tok1: float32 [256], replicated
- w_tok2: bfloat16 [256, 1024], replicated
- b_tok2: float32 [1024], replicated
- ln2_scale: float32 [512], replicated
- ln2_shift: float32 [512], replicated
- w_chan1: bfloat16 [512, 2048], replicated
- b_chan1: float32 [2048], replicated
- w_chan2: bfloat16 [2048, 512], replicated
- b_chan2: float32 [512], replicated
Outputs:
- output 1: bfloat16 [256, 1024, 512], P('data', 'seq'), parts along dimension 0
- output 2: bfloat16 [256, 1024, 512], P('data', 'seq'), parts along dimension 0
- output 3: float32 [4096, 256], P('data'), parts along dimension 0
- output 4: float32 [1024, 1024], P('data'), parts along dimension 0
- output 5: float32 [2048, 2048], P('data'), parts along dimension 0
- output 6: float32 [8192, 512], P('data'), parts along dimension 0
There are 4 independent parts. The reference program is written for one: setup_inputs(seed, part) draws one part's arguments, and reference() takes and returns one part's arrays. A program takes and returns all parts, laid end to end along the dimension named above; an argument that names none is the same for every part.
All inputs are finite; a program needn't handle non-finite values.
Results may differ from the reference program's by a relative error of at most 0.0167562.
Values are sent between devices in bfloat16 or wider.
A program may use at most 1 GiB of HBM per device.

```python
import jax
import jax.numpy as jnp
from jax import lax

IMAGES = 64
PATCHES = 1024
CHANNELS = 512
TOKEN_HID = 256
CHAN_HID = 2048

LN_EPS = 1e-6


def setup_inputs(seed: int = 0, part: int = 0) -> dict:
    part_key = jax.random.fold_in(jax.random.key(seed), part)
    act_key, grad_key = jax.random.split(part_key)
    weight_keys = jax.random.split(jax.random.key(seed + 1), 12)

    def draw_normal(key_index, shape, spread):
        return jax.random.normal(weight_keys[key_index], shape, jnp.float32) * spread

    act_in = jax.random.normal(act_key, (IMAGES, PATCHES, CHANNELS), jnp.float32)
    grad_out = jax.random.normal(grad_key, (IMAGES, PATCHES, CHANNELS), jnp.float32)
    return {
        "act_in": act_in.astype(jnp.bfloat16),
        "grad_out": grad_out.astype(jnp.bfloat16),
        "ln1_scale": 1.0 + draw_normal(0, (CHANNELS,), 0.3),
        "ln1_shift": draw_normal(1, (CHANNELS,), 0.3),
        "w_tok1": draw_normal(2, (PATCHES, TOKEN_HID), PATCHES ** -0.5).astype(jnp.bfloat16),
        "b_tok1": draw_normal(3, (TOKEN_HID,), 0.5),
        "w_tok2": draw_normal(4, (TOKEN_HID, PATCHES), TOKEN_HID ** -0.5).astype(jnp.bfloat16),
        "b_tok2": draw_normal(5, (PATCHES,), 0.5),
        "ln2_scale": 1.0 + draw_normal(6, (CHANNELS,), 0.3),
        "ln2_shift": draw_normal(7, (CHANNELS,), 0.3),
        "w_chan1": draw_normal(8, (CHANNELS, CHAN_HID), CHANNELS ** -0.5).astype(jnp.bfloat16),
        "b_chan1": draw_normal(9, (CHAN_HID,), 0.5),
        "w_chan2": draw_normal(10, (CHAN_HID, CHANNELS), CHAN_HID ** -0.5).astype(jnp.bfloat16),
        "b_chan2": draw_normal(11, (CHANNELS,), 0.5),
    }


def layer_norm(rows_in, ln_scale, ln_shift):
    widened = rows_in.astype(jnp.float32)
    row_mean = jnp.mean(widened, axis=-1, keepdims=True)
    centered = widened - row_mean
    row_var = jnp.mean(centered * centered, axis=-1, keepdims=True)
    return (centered * lax.rsqrt(row_var + LN_EPS) * ln_scale + ln_shift).astype(jnp.bfloat16)


def gelu_bf16(pre_act):
    return jax.nn.gelu(pre_act.astype(jnp.float32)).astype(jnp.bfloat16)


def reference(act_in, grad_out, ln1_scale, ln1_shift, w_tok1, b_tok1, w_tok2, b_tok2,
              ln2_scale, ln2_shift, w_chan1, b_chan1, w_chan2, b_chan2):
    def layer_forward(tok1_wide, tok2_wide, chan1_wide, chan2_wide, image):
        normed = layer_norm(image, ln1_scale, ln1_shift)
        tok_pre = (jnp.einsum("sd,sc->dc", tok1_wide, normed.astype(jnp.float32))
                   + b_tok1[:, None]).astype(jnp.bfloat16)
        tok_act = gelu_bf16(tok_pre)
        tok_out = (jnp.einsum("ds,dc->sc", tok2_wide, tok_act.astype(jnp.float32))
                   + b_tok2[:, None]).astype(jnp.bfloat16)
        mid_act = (image.astype(jnp.float32) + tok_out.astype(jnp.float32)).astype(jnp.bfloat16)
        normed_mid = layer_norm(mid_act, ln2_scale, ln2_shift)
        chan_pre = (jnp.einsum("sc,ch->sh", normed_mid.astype(jnp.float32), chan1_wide)
                    + b_chan1).astype(jnp.bfloat16)
        chan_act = gelu_bf16(chan_pre)
        chan_out = jnp.einsum("sh,hc->sc", chan_act.astype(jnp.float32), chan2_wide) + b_chan2
        return (mid_act.astype(jnp.float32) + chan_out).astype(jnp.bfloat16)

    tok1_wide = w_tok1.astype(jnp.float32)
    tok2_wide = w_tok2.astype(jnp.float32)
    chan1_wide = w_chan1.astype(jnp.float32)
    chan2_wide = w_chan2.astype(jnp.float32)

    def image_step(grad_sums, image_pair):
        image, image_grad = image_pair
        image_out, pullback = jax.vjp(layer_forward, tok1_wide, tok2_wide, chan1_wide, chan2_wide, image)
        cotangents = pullback(image_grad)
        new_sums = tuple(total + piece for total, piece in zip(grad_sums, cotangents[:4]))
        return new_sums, (image_out, cotangents[4])

    zero_sums = (jnp.zeros(w_tok1.shape, jnp.float32), jnp.zeros(w_tok2.shape, jnp.float32),
                 jnp.zeros(w_chan1.shape, jnp.float32), jnp.zeros(w_chan2.shape, jnp.float32))
    weight_sums, (act_out, grad_in) = lax.scan(image_step, zero_sums, (act_in, grad_out))
    return act_out, grad_in, weight_sums[0], weight_sums[1], weight_sums[2], weight_sums[3]
```

```python
import functools

import jax
import jax.numpy as jnp
from jax import lax
from jax.experimental import pallas as pl
from jax.experimental.pallas import tpu as pltpu
from jax.sharding import PartitionSpec as P


LN_EPS = 1e-6
F32 = jnp.float32
BF16 = jnp.bfloat16
GELU_C = 0.7978845608028654
GELU_C2 = GELU_C * 0.044715
GELU_C3 = 3.0 * GELU_C2
VMEM_LIMIT = 40 * 1024 * 1024
CHUNKS = (4,) + (8,) * 7 + (4,)


def norm_stats(wide):
    centered = wide - jnp.mean(wide, axis=-1, keepdims=True)
    var = jnp.mean(centered * centered, axis=-1, keepdims=True)
    return centered, lax.rsqrt(var + LN_EPS)


def norm_back(xhat, rstd, ct, scale):
    dxhat = ct * scale
    m1 = jnp.mean(dxhat, axis=-1, keepdims=True)
    m2 = jnp.mean(dxhat * xhat, axis=-1, keepdims=True)
    return rstd * (dxhat - m1 - xhat * m2)


def gelu_parts(pre):
    sq = pre * pre
    th = jnp.tanh(pre * (GELU_C + GELU_C2 * sq))
    return th, sq


def gelu_slope(pre, th, sq):
    half = 0.5 * pre
    return 0.5 + 0.5 * th + ((1.0 - th * th) * half) * (GELU_C + GELU_C3 * sq)


def dot(a, b):
    return jnp.dot(a, b, preferred_element_type=F32)


def dot_nt(a, b):
    return lax.dot_general(a, b, (((1,), (1,)), ((), ())), preferred_element_type=F32)


def col(block):
    return pl.ds(pl.multiple_of(block * 128, 128), 128)


def cost(flops, nbytes, trans=0):
    return pl.CostEstimate(flops=int(flops), bytes_accessed=int(nbytes), transcendentals=int(trans))


def params():
    return pltpu.CompilerParams(vmem_limit_bytes=VMEM_LIMIT, dimension_semantics=("arbitrary",))


def ln1_kernel(me_ref, x_ref, sc_ref, sh_ref, o0, o1, o2, o3, u_scr):
    me = me_ref[0]
    nb = x_ref.shape[0]
    for b in range(nb):
        wide = x_ref[b].astype(F32)
        cen, rstd = norm_stats(wide)
        u_scr[b] = (cen * rstd * sc_ref[...] + sh_ref[...]).astype(BF16)
    for k, o in enumerate((o0, o1, o2, o3)):
        o[...] = u_scr[:, :, col(me ^ k)]


def ln1_call(me, x, first, n, scale, shift, ib=4):
    s, c = x.shape[1:]
    base = first // ib
    piece = jax.ShapeDtypeStruct((n, s, 128), BF16)
    return pl.pallas_call(
        ln1_kernel,
        grid_spec=pltpu.PrefetchScalarGridSpec(
            num_scalar_prefetch=1,
            grid=(n // ib,),
            in_specs=[
                pl.BlockSpec((ib, s, c), lambda i, m: (base + i, 0, 0)),
                pl.BlockSpec((1, c), lambda i, m: (0, 0)),
                pl.BlockSpec((1, c), lambda i, m: (0, 0)),
            ],
            out_specs=[pl.BlockSpec((ib, s, 128), lambda i, m: (i, 0, 0))] * 4,
            scratch_shapes=[pltpu.VMEM((ib, s, c), BF16)],
        ),
        out_shape=[piece] * 4,
        compiler_params=params(),
        cost_estimate=cost(n * s * c * 60, n * s * c * 4),
        name="ln1_split",
    )(me, x, scale, shift)


def tok1_kernel(u0, u1, u2, u3, w_ref, b_ref, *rest):
    h_ref, g_ref = rest[-2:]
    nb = u0.shape[0]
    cols = [jnp.concatenate([u[b] for b in range(nb)], axis=1) for u in (u0, u1, u2, u3)]
    full = jnp.concatenate(cols, axis=0)
    h = (dot(w_ref[...], full) + b_ref[...]).astype(BF16)
    hw = h.astype(F32)
    th, _ = gelu_parts(hw)
    g = (0.5 * hw * (1.0 + th)).astype(BF16)
    for b in range(nb):
        h_ref[b] = h[:, b * 128:(b + 1) * 128]
        g_ref[b] = g[:, b * 128:(b + 1) * 128]


def tok1_call(pieces, w1p, b1, after=(), ib=4):
    n, s, _ = pieces[0].shape
    d = w1p.shape[0]
    spec = pl.BlockSpec((ib, s, 128), lambda i: (i, 0, 0))
    ospec = pl.BlockSpec((ib, d, 128), lambda i: (i, 0, 0))
    piece = jax.ShapeDtypeStruct((n, d, 128), BF16)
    return pl.pallas_call(
        tok1_kernel,
        grid=(n // ib,),
        in_specs=[spec] * 4 + [pl.BlockSpec(w1p.shape, lambda i: (0, 0)), pl.BlockSpec((d, 1), lambda i: (0, 0))]
        + [pl.BlockSpec(memory_space=pl.ANY)] * len(after),
        out_specs=[ospec] * 2,
        out_shape=[piece] * 2,
        compiler_params=params(),
        cost_estimate=cost(2 * n * 128 * 4 * s * d, n * s * 128 * 12),
        name="tok1",
    )(*pieces, w1p, b1, *after)


def chan_kernel(has_acc, me_ref, x_ref, dz_ref, g0, g1, g2, g3, w2l_ref, bt2_ref, sc_ref, sh_ref, w1_ref, w1t_ref,
                b1_ref, w2_ref, w2t_ref, b2_ref, *rest):
    if has_acc:
        a1, a2, a3, _, *rest = rest
    z_ref, m0, m1, m2, m3, gw1, gw2, gt2, g_scr, q_scr, da_scr, dm_scr = rest
    me = me_ref[0]
    nb, s, _ = x_ref.shape

    @pl.when(pl.program_id(0) == 0)
    def _():
        if not has_acc:
            gw1[...] = jnp.zeros_like(gw1)
            gw2[...] = jnp.zeros_like(gw2)
            gt2[...] = jnp.zeros_like(gt2)

    for k, g in enumerate((g0, g1, g2, g3)):
        g_scr[:, :, col(me ^ k)] = g[...]
    mids = []
    for b in range(nb):
        t = (dot(w2l_ref[...], g_scr[b]) + bt2_ref[...]).astype(BF16)
        mids.append((x_ref[b].astype(F32) + t.astype(F32)).astype(BF16))
    mid = jnp.concatenate(mids, axis=0).astype(F32)
    cen, rstd = norm_stats(mid)
    xhat = cen * rstd
    v = (xhat * sc_ref[...] + sh_ref[...]).astype(BF16)
    dz = jnp.concatenate([dz_ref[b] for b in range(nb)], axis=0)
    hid = w1_ref.shape[1]
    step = 512
    for j in range(hid // step):
        sl = slice(j * step, (j + 1) * step)
        a = (dot(v, w1_ref[:, sl]) + b1_ref[:, sl]).astype(BF16).astype(F32)
        dq = dot(dz, w2t_ref[:, sl]).astype(BF16).astype(F32)
        th, sq = gelu_parts(a)
        q_scr[:, sl] = (0.5 * a * (1.0 + th)).astype(BF16)
        da_scr[:, sl] = (dq * gelu_slope(a, th, sq)).astype(BF16)
    vt = v.T
    dzt = dz.T
    dv = dot(da_scr[...], w1t_ref[...]).astype(BF16).astype(F32)
    gw1[...] += dot(vt, da_scr[...])
    dmid = (dz.astype(F32) + norm_back(xhat, rstd, dv, sc_ref[...]).astype(BF16).astype(F32)).astype(BF16)
    z = (mid + (dot(q_scr[...], w2_ref[...]) + b2_ref[...])).astype(BF16)
    gw2[...] += dot(dzt, q_scr[...])
    tok = gt2[...]
    for b in range(nb):
        rows = slice(b * s, (b + 1) * s)
        z_ref[b] = z[rows]
        dm_scr[b] = dmid[rows]
        tok += dot_nt(g_scr[b], dmid[rows])
    gt2[...] = tok
    for k, m in enumerate((m0, m1, m2, m3)):
        m[...] = dm_scr[:, :, col(me ^ k)]


def chan_call(me, x, dz, first, n, gs, w2l, bt2, scale, shift, w1, w1t, b1, w2, w2t, b2, prev, ib=2):
    s, c = x.shape[1:]
    d = gs[0].shape[1]
    hid = w1.shape[1]
    base = first // ib
    one = pl.Buffered(1)

    def whole(arr):
        return pl.BlockSpec(arr.shape, lambda i, m: (0,) * arr.ndim, pipeline_mode=one)

    consts = (w2l, bt2, scale, shift, w1, w1t, b1, w2, w2t, b2)
    acc_shapes = [pltpu.VMEM((c, hid), F32), pltpu.VMEM((c, hid), F32), pltpu.VMEM((d, s), F32)]
    rows = pl.BlockSpec((ib, s, c), lambda i, m: (base + i, 0, 0))
    vmem = pl.BlockSpec(memory_space=pltpu.VMEM)
    in_specs = [rows, rows] + [pl.BlockSpec((ib, d, 128), lambda i, m: (i, 0, 0))] * 4 + [
        vmem if a.size >= c * hid else whole(a) for a in consts]
    extra, aliases = (), {}
    if prev:
        z_prev, accs = prev
        extra = tuple(accs) + (z_prev,)
        in_specs += [vmem] * 3 + [pl.BlockSpec(memory_space=pl.ANY)]
        aliases = {len(in_specs): 0, len(in_specs) - 3: 5, len(in_specs) - 2: 6, len(in_specs) - 1: 7}
    return pl.pallas_call(
        functools.partial(chan_kernel, bool(prev)),
        grid_spec=pltpu.PrefetchScalarGridSpec(
            num_scalar_prefetch=1,
            grid=(n // ib,),
            in_specs=in_specs,
            out_specs=[rows] + [pl.BlockSpec((ib, s, 128), lambda i, m: (i, 0, 0))] * 4 + [vmem] * 3,
            scratch_shapes=[
                pltpu.VMEM((ib, d, c), BF16),
                pltpu.VMEM((ib * s, hid), BF16),
                pltpu.VMEM((ib * s, hid), BF16),
                pltpu.VMEM((ib, s, c), BF16),
            ],
        ),
        out_shape=[jax.ShapeDtypeStruct(x.shape, BF16)] + [jax.ShapeDtypeStruct((n, s, 128), BF16)] * 4 + acc_shapes,
        input_output_aliases=aliases,
        compiler_params=params(),
        cost_estimate=cost(12 * n * s * c * hid, n * s * c * 10 + 24 * 2**20, n * s * hid),
        name="chan",
    )(me, x, dz, *gs, *consts, *extra)


def tok_back_kernel(t0, t1, t2, t3, w_ref, h_ref, o_ref):
    nb = t0.shape[0]
    cols = [jnp.concatenate([t[b] for b in range(nb)], axis=1) for t in (t0, t1, t2, t3)]
    full = jnp.concatenate(cols, axis=0)
    dg = dot(w_ref[...], full).astype(BF16).astype(F32)
    h = jnp.concatenate([h_ref[b] for b in range(nb)], axis=1).astype(F32)
    th, sq = gelu_parts(h)
    dh = (dg * gelu_slope(h, th, sq)).astype(BF16)
    for b in range(nb):
        o_ref[b] = dh[:, b * 128:(b + 1) * 128]


def tok_back_call(pieces, w2p, h, ib=4):
    n, s, _ = pieces[0].shape
    d = w2p.shape[0]
    spec = pl.BlockSpec((ib, s, 128), lambda i: (i, 0, 0))
    ospec = pl.BlockSpec((ib, d, 128), lambda i: (i, 0, 0))
    return pl.pallas_call(
        tok_back_kernel,
        grid=(n // ib,),
        in_specs=[spec] * 4 + [pl.BlockSpec(w2p.shape, lambda i: (0, 0)), ospec],
        out_specs=ospec,
        out_shape=jax.ShapeDtypeStruct((n, d, 128), BF16),
        compiler_params=params(),
        cost_estimate=cost(2 * n * 128 * 4 * s * d, n * s * 128 * 12),
        name="tok_back",
    )(*pieces, w2p, h)


def fin_kernel(has_acc, n_after, me_ref, x_ref, m0, m1, m2, m3, h0, h1, h2, h3, w_ref, sc_ref, sh_ref, *rest):
    if has_acc:
        a1, _, *rest = rest
    dx_ref, gt1, h_scr, m_scr = rest[n_after:]
    me = me_ref[0]
    nb, _, _ = x_ref.shape

    @pl.when(pl.program_id(0) == 0)
    def _():
        gt1[...] = a1[...] if has_acc else jnp.zeros_like(gt1)

    for k, (h, m) in enumerate(zip((h0, h1, h2, h3), (m0, m1, m2, m3))):
        h_scr[:, :, col(me ^ k)] = h[...]
        m_scr[:, :, col(me ^ k)] = m[...]
    tok = gt1[...]
    for b in range(nb):
        dh = h_scr[b]
        du = dot(w_ref[...], dh).astype(BF16).astype(F32)
        cen, rstd = norm_stats(x_ref[b].astype(F32))
        xhat = cen * rstd
        u = (xhat * sc_ref[...] + sh_ref[...]).astype(BF16)
        dln = norm_back(xhat, rstd, du, sc_ref[...]).astype(BF16)
        dx_ref[b] = (m_scr[b].astype(F32) + dln.astype(F32)).astype(BF16)
        tok += dot_nt(u, dh)
    gt1[...] = tok


def fin_call(me, x, dms, first, n, dhs, w1l, scale, shift, prev, after=(), ib=4):
    s, c = x.shape[1:]
    d = dhs[0].shape[1]
    base = first // ib
    consts = (w1l, scale, shift)

    def whole(arr):
        return pl.BlockSpec(arr.shape, lambda i, m: (0,) * arr.ndim)

    acc_shape = jax.ShapeDtypeStruct((s, d), F32)
    rows = pl.BlockSpec((ib, s, c), lambda i, m: (base + i, 0, 0))
    in_specs = ([rows] + [pl.BlockSpec((ib, s, 128), lambda i, m: (i, 0, 0))] * 4
                + [pl.BlockSpec((ib, d, 128), lambda i, m: (i, 0, 0))] * 4 + [whole(a) for a in consts])
    extra, aliases = (), {}
    if prev:
        dx_prev, acc = prev
        extra = (acc, dx_prev)
        in_specs += [whole(acc), pl.BlockSpec(memory_space=pl.ANY)]
        aliases = {len(in_specs): 0}
    extra += tuple(after)
    in_specs += [pl.BlockSpec(memory_space=pl.ANY)] * len(after)
    return pl.pallas_call(
        functools.partial(fin_kernel, bool(prev), len(after)),
        grid_spec=pltpu.PrefetchScalarGridSpec(
            num_scalar_prefetch=1,
            grid=(n // ib,),
            in_specs=in_specs,
            out_specs=[rows, whole(acc_shape)],
            scratch_shapes=[pltpu.VMEM((ib, d, c), BF16), pltpu.VMEM((ib, s, c), BF16)],
        ),
        out_shape=[jax.ShapeDtypeStruct(x.shape, BF16), acc_shape],
        input_output_aliases=aliases,
        compiler_params=params(),
        cost_estimate=cost(4 * n * s * c * d + n * s * c * 60, n * s * c * 8),
        name="fin",
    )(me, x, *dms, *dhs, *consts, *extra)


def place_kernel(me_ref, m_ref, o_ref, *rest):
    g1_ref, g2_ref = rest[-2:]
    even = (me_ref[0] % 2) == 0
    mine, other = m_ref[...], o_ref[...]
    g1_ref[...] = jnp.where(even, mine, other)
    g2_ref[...] = jnp.where(even, other, mine).T


def place_call(me, mine, other, part, c, prev):
    rows, hid = mine.shape
    spec = pl.BlockSpec((rows, hid), lambda i, m: (0, 0))
    hbm = pl.BlockSpec(memory_space=pl.ANY)
    return pl.pallas_call(
        place_kernel,
        grid_spec=pltpu.PrefetchScalarGridSpec(
            num_scalar_prefetch=1,
            grid=(1,),
            in_specs=[spec, spec] + [hbm] * len(prev),
            out_specs=[pl.BlockSpec((rows, hid), lambda i, m: (part, 0)), pl.BlockSpec((hid, rows), lambda i, m: (0, part))],
        ),
        out_shape=[jax.ShapeDtypeStruct((c, hid), F32), jax.ShapeDtypeStruct((hid, c), F32)],
        input_output_aliases={3: 0, 4: 1} if prev else {},
        compiler_params=params(),
        cost_estimate=cost(rows * hid * 20, rows * hid * 16),
        name="place",
    )(me, mine, other, *prev)


PARTS = 4


def solution(mesh):
    act_spec = P("data", "seq", None)
    part_spec = P("data", None)
    spec_in = (act_spec, act_spec) + (P(),) * 12
    spec_out = (act_spec, act_spec, part_spec, part_spec, part_spec, part_spec)

    def swap(arr, k):
        return lax.ppermute(arr, "seq", [(i, i ^ k) for i in range(4)])

    def exchange(pieces):
        return (pieces[0],) + tuple(swap(pieces[k], k) for k in (1, 2, 3))

    def gather(own):
        far = swap(own, 2)
        return own, swap(own, 1), far, swap(far, 1)

    def device_step(act, grad, ln1_scale, ln1_shift, w_tok1, b_tok1, w_tok2, b_tok2,
                    ln2_scale, ln2_shift, w_chan1, b_chan1, w_chan2, b_chan2):
        s = act.shape[1]
        me = lax.axis_index("seq")
        me1 = me.astype(jnp.int32)[None]
        sc1, sh1, sc2, sh2 = (a[None, :] for a in (ln1_scale, ln1_shift, ln2_scale, ln2_shift))
        w1l = lax.dynamic_slice_in_dim(w_tok1, me * s, s, 0)
        w2l = lax.dynamic_slice_in_dim(w_tok2, me * s, s, 1).T
        bt2 = lax.dynamic_slice_in_dim(b_tok2, me * s, s, 0)[:, None]
        w1p = jnp.concatenate([lax.dynamic_slice_in_dim(w_tok1, (me ^ k) * s, s, 0) for k in range(4)], axis=0).T
        w2p = jnp.concatenate([lax.dynamic_slice_in_dim(w_tok2, (me ^ k) * s, s, 1) for k in range(4)], axis=1)
        w_chan1, w1t, w_chan2, w2t = (
            pltpu.with_memory_space_constraint(w, pltpu.VMEM) for w in (w_chan1, w_chan1.T, w_chan2, w_chan2.T))
        bt1, b1, b2 = b_tok1[:, None], b_chan1[None, :], b_chan2[None, :]

        n = len(CHUNKS)
        starts = [sum(CHUNKS[:i]) for i in range(n)]
        us, hs, gs, dms, dts = [], [], [], [], []

        def ln_step(i):
            pieces = ln1_call(me1, act, starts[i], CHUNKS[i], sc1, sh1)
            us.append(exchange(pieces))

        def tok_step(i):
            h, g = tok1_call(us[i], w1p, bt1, (w1t, w2t) if i == 0 else ())
            hs.append(h)
            gs.append(gather(g))

        for i in range(n):
            ln_step(i)
        for i in range(n):
            tok_step(i)
        prev = None
        for i in range(n):
            z, *rest = chan_call(me1, act, grad, starts[i], CHUNKS[i], gs[i], w2l, bt2, sc2, sh2, w_chan1, w1t, b1,
                                 w_chan2, w2t, b2, prev)
            prev = (z, rest[4:])
            dms.append(rest[:4])
            dts.append(exchange(rest[:4]))
        gw1, gw2t, gt2 = prev[1]
        dhs = []
        for i in range(n):
            dh = tok_back_call(dts[i], w2p, hs[i])
            dhs.append(gather(dh))

        def spread(own, axis):
            out = jnp.concatenate([own] * 4, axis=axis)
            for k, p in enumerate(gather(own)):
                out = lax.dynamic_update_slice_in_dim(out, p, (me ^ k) * s, axis)
            return out

        gt2 = spread(gt2, 1)
        even = (me % 2) == 0
        rows = gw1.shape[0] // PARTS
        sums = []
        for h in range(PARTS):
            p1, p2 = (g[h * rows:(h + 1) * rows] for g in (gw1, gw2t))
            mine, other = jnp.where(even, p1, p2), jnp.where(even, p2, p1)
            mine = mine + swap(other, 1)
            mine = mine + swap(mine, 2)
            sums.append((mine, swap(mine, 1)))

        prev = None
        for i in range(n):
            after = (gt2,) if i == n - 1 else ()
            prev = fin_call(me1, act, dms[i], starts[i], CHUNKS[i], dhs[i], w1l, sc1, sh1, prev, after)
        dx, gt1 = prev
        prev, c = (), gw1.shape[0]
        for h in range(PARTS):
            prev = place_call(me1, *sums[h], h, c, prev)
        gw1, gw2 = prev

        return z, dx, spread(gt1, 0), gt2, gw1, gw2

    return jax.shard_map(device_step, mesh=mesh, in_specs=spec_in, out_specs=spec_out, check_vma=False)
```
